32 devices in a mesh: image: 4 (over y, x), band: 2 (over core), ga: 4 (over z).
Axes of the slice: x: 2, y: 2, z: 4, core: 2. Of those that a mesh axis runs over, the one named last changes fastest.
Arguments:
- wave_coeffs: bfloat16 [4, 64, 2, 262144], P('image', 'band', None, 'ga'), may hold values from -6 to 6
- occupation: float32 [4, 64], P('image', 'band'), may hold values from 0.003125 to 0.0625
- form_factor: float32 [4, 8, 262144], P(None, None, 'ga'), may hold values from -0.005859375 to 0.005859375
- g_vectors: float32 [3, 262144], P(None, 'ga'), may hold values from -2 to 2
- species: int32 [64], replicated, may hold values from 0 to 3
- proj_count: int32 [4], replicated, may hold values from 1 to 8, as said below
- coupling: float32 [4, 8], replicated, may hold values from 0.5 to 2.5
- positions: float32 [4, 3, 64], P('image'), may hold values from -5.4 to 29.4, as said below
- energy_rest: float32 [4], P('image'), may hold values from -8 to 8
- force_rest: float32 [4, 3, 64], P('image'), may hold values from -6 to 6
- end_positions: float32 [2, 3, 64], replicated, may hold values from -5.4 to 29.4, as said below
- end_energy: float32 [2], replicated, may hold values from -8 to 8
- climb_index: int32 [1], replicated, may hold values from 0 to 3
- tangent_kind: int32 [4], P('image'), may hold values from 0 to 3
Outputs:
- neb_force: float32 [4, 3, 64], P('image')
- energy: float32 [4], P('image')
The draws below stay inside these ranges and needn't reach their ends.
Inputs may be any that keep to these rules, and one draw needn't show every extreme that they name: `proj_count`: each species has between 1 and 8 live projector slots, and some species has exactly 8. `positions`: atom coordinates in bohr. `end_positions`: atom coordinates in bohr.
All inputs are finite; a program needn't handle non-finite values.
Results may differ from the reference program's by a relative error of at most 0.0003.
The reference program's roundings to bfloat16 on the way (of `projector` and `stacked`) count: a program that leaves them out, or rounds other values in their place, can miss the bound.
Values sent between devices are 32-bit elements; how exact they have to be, the bound alone decides.
A program may use at most 128 MiB of HBM per device.

```python
import jax
import jax.numpy as jnp
from jax import lax

NG = 262144
ATOMS = 64
PMAX = 8
SPECIES = 4
IMG = 4
BANDS = 64
N_GA = 4


def chain_path(key):
    base_key = jax.random.fold_in(key, 11)
    step_key = jax.random.fold_in(key, 12)
    base = jax.random.uniform(base_key, (3, ATOMS), jnp.float32, 0.0, 24.0)
    steps = 0.3 * jnp.clip(jax.random.normal(step_key, (IMG + 2, 3, ATOMS), jnp.float32), -3.0, 3.0)
    return base[None, :, :] + jnp.cumsum(steps, axis=0)


def draw_positions(key, part):
    return chain_path(key)[1:IMG + 1]


def draw_end_positions(key, part):
    path = chain_path(key)
    return jnp.stack([path[0], path[IMG + 1]], axis=0)


def draw_proj_count(key, part):
    counts = jax.random.randint(jax.random.fold_in(key, 21), (SPECIES,), 1, PMAX + 1, jnp.int32)
    filled = jax.random.randint(jax.random.fold_in(key, 22), (), 0, SPECIES, jnp.int32)
    return jnp.where(jnp.arange(SPECIES, dtype=jnp.int32) == filled, PMAX, counts).astype(jnp.int32)


def place_ends(drawn, rng, smallest, high):
    shape = drawn.shape
    spot = [jax.random.randint(jax.random.fold_in(rng, axis), (), 0, shape[axis]) for axis in range(len(shape))]
    drawn = drawn.at[tuple(spot)].set(smallest)
    longest = shape.index(max(shape))
    spot[longest] = (spot[longest] + 1) % shape[longest]
    return drawn.at[tuple(spot)].set(high)


def levels(stream_key, extent, cuts, low, top_value):
    loudness = 1.0
    for dim, blocks in cuts:
        steps = jax.random.uniform(jax.random.fold_in(jax.random.fold_in(stream_key, 6), dim), (blocks,), jnp.float32, low / len(cuts), top_value / len(cuts))
        loudness = loudness * jnp.repeat(jnp.exp(steps), extent[dim] // blocks).reshape((-1,) + (1,) * (len(extent) - 1 - dim))
    return loudness


def centred(stream_key, dims, deviation, limit, cuts=(), kind=jnp.bfloat16):
    array = jax.random.normal(stream_key, dims, jnp.float32) * deviation
    if len(cuts) > 0:
        array = levels(stream_key, dims, cuts, -0.22, 0.18) * array
    return jnp.clip(array, min=-limit, max=limit).astype(kind)


def setup_inputs(seed: int = 0) -> dict:
    key_of = jax.random.split(jax.random.key(seed), 15)
    return {
        "wave_coeffs": centred(key_of[0], (IMG, BANDS, 2, NG), 1.0, 6.0, ((0, 4), (1, 2), (3, 4))),
        "occupation": jnp.clip(0.003125 + 0.059375 * jax.random.uniform(key_of[1], (IMG, BANDS), jnp.float32) ** levels(key_of[1], (IMG, BANDS), ((0, 4), (1, 2)), -0.2, 0.2), 0.003125, 0.0625),
        "form_factor": centred(key_of[2], (SPECIES, PMAX, NG), (4 * NG) ** -0.5, 0.005859375, ((2, 4),), jnp.float32),
        "g_vectors": jnp.clip(jax.random.uniform(key_of[3], (3, NG), jnp.float32, -2.0, 2.0) * levels(key_of[3], (3, NG), ((1, 4),), -0.4, 0.0), -2.0, 2.0),
        "species": place_ends(jax.random.randint(key_of[4], (ATOMS,), 0, SPECIES), jax.random.fold_in(key_of[4], 1), 0, SPECIES - 1).astype(jnp.int32),
        "proj_count": draw_proj_count(jax.random.fold_in(key_of[14], 71), 0),
        "coupling": jnp.clip(jax.random.uniform(key_of[6], (SPECIES, PMAX), jnp.float32, 0.5, 2.5), 0.5, 2.5),
        "positions": draw_positions(jax.random.fold_in(key_of[14], 71), 0),
        "energy_rest": centred(key_of[8], (IMG,), 2.0, 8.0, ((0, 4),), jnp.float32),
        "force_rest": centred(key_of[9], (IMG, 3, ATOMS), 1.0, 6.0, ((0, 4),), jnp.float32),
        "end_positions": draw_end_positions(jax.random.fold_in(key_of[14], 71), 0),
        "end_energy": centred(key_of[11], (2,), 2.0, 8.0, (), jnp.float32),
        "climb_index": jax.random.randint(key_of[12], (1,), 0, IMG).astype(jnp.int32),
        "tangent_kind": place_ends(jax.random.randint(key_of[13], (IMG,), 0, 4), jax.random.fold_in(key_of[13], 1), 0, 3).astype(jnp.int32),
    }


spring_constant = 5.0

def atom_tables(species, proj_count, coupling):
    is_species = (species[:, None] == jnp.arange(SPECIES)[None, :]).astype(jnp.float32)
    is_live = (jnp.arange(PMAX)[None, :] < proj_count[:, None]).astype(jnp.float32)
    species_mask = is_species[:, :, None] * is_live[None, :, :]
    strength = lax.optimization_barrier(jnp.sum(species_mask * coupling[None, :, :], axis=1))
    return (species_mask, strength)

def projectors(atom_pos, species_mask, form_factor, g_vectors):
    phases = atom_pos[0][:, None] * g_vectors[0][None, :]
    phases = phases + atom_pos[1][:, None] * g_vectors[1][None, :]
    phases = phases + atom_pos[2][:, None] * g_vectors[2][None, :]
    cosine = jnp.cos(phases)
    sine_part = jnp.sin(phases)
    radial = species_mask[:, 0, :, None] * form_factor[0][None, :, :]
    for spec_num in range(1, SPECIES):
        radial = radial + species_mask[:, spec_num, :, None] * form_factor[spec_num][None, :, :]
    real_part = radial * cosine[:, None, :]
    imag_part = -radial * sine_part[:, None, :]
    joined = jnp.concatenate([real_part, imag_part], axis=-1).astype(jnp.bfloat16)
    return joined.reshape(joined.shape[0] * joined.shape[1], joined.shape[2])

def stack_waves(waves_here, g_vectors):
    band_count = waves_here.shape[0]
    real_part = waves_here[:, 0, :].astype(jnp.float32)
    imag_part = waves_here[:, 1, :].astype(jnp.float32)
    pieces = [waves_here.reshape(band_count, 2 * waves_here.shape[2])]
    for axis_num in range(3):
        direction = g_vectors[axis_num][None, :]
        pieces.append(jnp.concatenate([-direction * imag_part, direction * real_part], axis=-1).astype(jnp.bfloat16))
    return jnp.concatenate(pieces, axis=0)

def contract(projector, stacked):
    return 2.0 * lax.dot_general(projector, stacked, (((1,), (1,)), ((), ())), preferred_element_type=jnp.float32)

def nonlocal_terms(proj_sums, occupied, strength):
    band_count = occupied.shape[0]
    atom_count = strength.shape[0]
    intersect = proj_sums[:, :band_count]
    weighted = intersect * occupied[None, :]
    energy_part = jnp.sum(strength.reshape(-1) * lax.optimization_barrier(jnp.sum(weighted * intersect, axis=1)))
    forces = []
    for axis_num in range(3):
        slope = proj_sums[:, (axis_num + 1) * band_count:(axis_num + 2) * band_count]
        per_row = lax.optimization_barrier(jnp.sum(weighted * slope, axis=1)).reshape(atom_count, PMAX)
        forces.append(-2.0 * lax.optimization_barrier(jnp.sum(strength * per_row, axis=1)))
    return (energy_part, jnp.stack(forces, axis=0))

def neb_project(force, here, prev_pos, next_pos, energy, prev_energy, next_energy, tangent_kind, is_climb):
    to_next = next_pos - here
    from_prev = here - prev_pos
    rise_next = jnp.abs(next_energy - energy)
    rise_prev = jnp.abs(prev_energy - energy)
    larger = jnp.maximum(rise_next, rise_prev)
    smaller = jnp.minimum(rise_next, rise_prev)
    rising = next_energy > prev_energy
    weight_next = 1.0 + jnp.where(rising, larger, smaller)
    weight_prev = 1.0 + jnp.where(rising, smaller, larger)
    stiff_next = spring_constant * (1.0 + jax.nn.sigmoid(0.5 * (next_energy + energy)))
    stiff_prev = spring_constant * (1.0 + jax.nn.sigmoid(0.5 * (prev_energy + energy)))
    length_next = jnp.sqrt(lax.optimization_barrier(jnp.sum(to_next * to_next, axis=(1, 2))) + 1.0)
    length_prev = jnp.sqrt(lax.optimization_barrier(jnp.sum(from_prev * from_prev, axis=(1, 2))) + 1.0)
    upwind = weight_next[:, None, None] * to_next + weight_prev[:, None, None] * from_prev
    forward = to_next / length_next[:, None, None]
    backward = from_prev / length_prev[:, None, None]
    kind = tangent_kind[:, None, None]
    tangent = jnp.where(kind == 0, upwind, jnp.where(kind == 1, forward + backward, jnp.where(kind == 2, forward, backward)))
    unit_tangent = tangent / jnp.sqrt(lax.optimization_barrier(jnp.sum(tangent * tangent, axis=(1, 2))) + 1.0)[:, None, None]
    along = lax.optimization_barrier(jnp.sum(force * unit_tangent, axis=(1, 2)))[:, None, None]
    climbing = force - 2.0 * along * unit_tangent
    regular = force - along * unit_tangent + (stiff_next * length_next - stiff_prev * length_prev)[:, None, None] * unit_tangent
    return jnp.where(is_climb[:, None, None], climbing, regular)

def reference(wave_coeffs, occupation, form_factor, g_vectors, species, proj_count, coupling, positions, energy_rest, force_rest, end_positions, end_energy, climb_index, tangent_kind):
    species_mask, strength = atom_tables(species, proj_count, coupling)
    block_len = NG // N_GA
    energies = []
    forces = []
    for image_num in range(IMG):
        waves_image = wave_coeffs[image_num]
        atom_pos = positions[image_num]

        def accumulate(block_num, total):
            start = (block_num * block_len).astype(jnp.int32)
            waves_block = lax.dynamic_slice_in_dim(waves_image, start, block_len, 2)
            form_block = lax.dynamic_slice_in_dim(form_factor, start, block_len, 2)
            g_block = lax.dynamic_slice_in_dim(g_vectors, start, block_len, 1)
            stacked = stack_waves(waves_block, g_block)
            projector = projectors(atom_pos, species_mask, form_block, g_block)
            return total + contract(projector, stacked)
        initial = jnp.zeros((ATOMS * PMAX, 4 * BANDS), jnp.float32)
        proj_sums = lax.fori_loop(0, N_GA, accumulate, initial)
        energy_part, force_part = nonlocal_terms(proj_sums, occupation[image_num], strength)
        energies.append(energy_part)
        forces.append(force_part)
    energy = energy_rest + jnp.stack(energies)
    force = force_rest + jnp.stack(forces, axis=0)
    chain_pos = jnp.concatenate([end_positions[:1], positions, end_positions[1:]], axis=0)
    chain_energy = jnp.concatenate([end_energy[:1], energy, end_energy[1:]], axis=0)
    is_climb = jnp.arange(IMG, dtype=jnp.int32) == climb_index[0]
    neb_force = neb_project(force, positions, chain_pos[:-2], chain_pos[2:], energy, chain_energy[:-2], chain_energy[2:], tangent_kind, is_climb)
    return (neb_force, energy)
```

```python
import math

import jax
import jax.numpy as jnp
from jax import lax
from jax.experimental import pallas as pl
from jax.experimental.pallas import tpu as pltpu
from jax.sharding import PartitionSpec as P

ATOMS = 64
PMAX = 8
SPECIES = 4


spring_constant = 5.0


def passed_along(array, axis, by):
    length = lax.axis_size(axis)
    pairs = [(i, i + by) for i in range(length) if 0 <= i + by < length]
    return lax.ppermute(array, axis, pairs)


def atom_tables(species, proj_count, coupling):
    is_species = (species[:, None] == jnp.arange(SPECIES)[None, :]).astype(jnp.float32)
    is_live = (jnp.arange(PMAX)[None, :] < proj_count[:, None]).astype(jnp.float32)
    species_mask = is_species[:, :, None] * is_live[None, :, :]
    strength = jnp.sum(species_mask * coupling[None, :, :], axis=1)
    return (species_mask, strength)


SIN_HALF = (0.7071067780965931, -0.02946276693049568, 0.00036827213876565137, -2.1885830267998076e-06, 7.194201360627222e-09)
COS_HALF = (-1.4142134949348355, 0.17677635430234293, -0.003682571658574129, 3.061195661905538e-05, -1.2786908538293617e-07)
TURN_HIGH = 6.28125
TURN_LOW = 0.001935307179586232
ROUNDER = 12582912.0
SUB = 1024
BLOCK = 8192
GROUP = 8


def horner(coefs, z):
    total = coefs[-1] * z + coefs[-2]
    for coef in coefs[-3::-1]:
        total = total * z + coef
    return total


def cos_and_minus_sin(phases):
    turns = (phases * 0.15915494309189535 + ROUNDER) - ROUNDER
    r = (phases - turns * TURN_HIGH) - turns * TURN_LOW
    z = r * r
    half_sin = r * horner(SIN_HALF, z)
    return (1.0 - half_sin * half_sin, half_sin * horner(COS_HALF, z))


def sums_kernel(spec_ref, w_ref, ff_ref, g_ref, pos_ref, live_ref, out_ref,
                acc, rad, stk, prj, trig):
    step = pl.program_id(0)
    rows = w_ref.shape[0]
    bands = rows // 2
    block = w_ref.shape[1]
    sub = stk.shape[1]
    groups = prj.shape[0]
    half = GROUP * PMAX

    @pl.when(step == 0)
    def _():
        acc[...] = jnp.zeros_like(acc)

    def wide(x):
        return jnp.concatenate([x] * (sub // 128), axis=1)

    def body(t, carry):
        lanes = pl.ds(pl.multiple_of(t * sub, sub), sub)
        for s in range(SPECIES):
            rad[s] = ff_ref[s, :, lanes] * wide(live_ref[s])
        w = w_ref[:, lanes]
        stk[0:rows, :] = w
        for c in range(3):
            stk[(c + 1) * rows : (c + 2) * rows, :] = (
                g_ref[c : c + 1, lanes] * w.astype(jnp.float32)
            ).astype(jnp.bfloat16)

        def multiply(j):
            acc[j] += lax.dot_general(
                prj[j], stk[...], (((1,), (1,)), ((), ())), preferred_element_type=jnp.float32
            )

        for j in range(groups):
            mine = slice(j * GROUP, (j + 1) * GROUP)
            phases = wide(pos_ref[0, mine, :]) * g_ref[0:1, lanes]
            phases = phases + wide(pos_ref[1, mine, :]) * g_ref[1:2, lanes]
            phases = phases + wide(pos_ref[2, mine, :]) * g_ref[2:3, lanes]
            cosine, minus_sine = cos_and_minus_sin(phases)
            trig[j, 0] = cosine
            trig[j, 1] = minus_sine
            for i in range(0, GROUP, 2):
                first = rad[spec_ref[j * GROUP + i]]
                second = rad[spec_ref[j * GROUP + i + 1]]
                for part in range(2):
                    pair = jnp.concatenate(
                        [first * trig[j, part, i : i + 1, :],
                         second * trig[j, part, i + 1 : i + 2, :]], axis=0)
                    at = part * half + i * PMAX
                    prj[j, at : at + 2 * PMAX, :] = pair.astype(jnp.bfloat16)
            if j > 0:
                multiply(j - 1)
        multiply(groups - 1)
        return carry

    lax.fori_loop(0, block // sub, body, 0)

    @pl.when(step == pl.num_programs(0) - 1)
    def _():
        for j in range(groups):
            real = acc[j, :half, :]
            imag = acc[j, half:, :]
            here = slice(j * half, (j + 1) * half)
            out_ref[here, 0:bands] = 2.0 * (real[:, :bands] + imag[:, bands:rows])
            for c in range(1, 4):
                out_ref[here, c * bands : (c + 1) * bands] = 2.0 * (
                    imag[:, c * rows : c * rows + bands]
                    - real[:, c * rows + bands : (c + 1) * rows]
                )


def projector_sums(waves, form_factor, g_vectors, species, proj_count, atom_pos):
    bands, _, length = waves.shape
    atoms = species.shape[0]
    w = jnp.swapaxes(waves, 0, 1).reshape(2 * bands, length)
    block = math.gcd(length, BLOCK)
    sub = math.gcd(block, SUB)
    groups = atoms // GROUP
    live = (jnp.arange(PMAX)[None, :] < proj_count[:, None]).astype(jnp.float32)
    live = jnp.broadcast_to(live[:, :, None], (SPECIES, PMAX, 128))
    pos = jnp.broadcast_to(atom_pos[:, :, None], (3, atoms, 128))
    grid_spec = pltpu.PrefetchScalarGridSpec(
        num_scalar_prefetch=1,
        grid=(length // block,),
        in_specs=[
            pl.BlockSpec((2 * bands, block), lambda i, sp: (0, i)),
            pl.BlockSpec((SPECIES, PMAX, block), lambda i, sp: (0, 0, i)),
            pl.BlockSpec((3, block), lambda i, sp: (0, i)),
            pl.BlockSpec((3, atoms, 128), lambda i, sp: (0, 0, 0)),
            pl.BlockSpec((SPECIES, PMAX, 128), lambda i, sp: (0, 0, 0)),
        ],
        out_specs=pl.BlockSpec((atoms * PMAX, 4 * bands), lambda i, sp: (0, 0)),
        scratch_shapes=[
            pltpu.VMEM((groups, 2 * GROUP * PMAX, 8 * bands), jnp.float32),
            pltpu.VMEM((SPECIES, PMAX, sub), jnp.float32),
            pltpu.VMEM((8 * bands, sub), jnp.bfloat16),
            pltpu.VMEM((groups, 2 * GROUP * PMAX, sub), jnp.bfloat16),
            pltpu.VMEM((groups, 2, GROUP, sub), jnp.float32),
        ],
    )
    return pl.pallas_call(
        sums_kernel,
        grid_spec=grid_spec,
        out_shape=jax.ShapeDtypeStruct((atoms * PMAX, 4 * bands), jnp.float32),
        compiler_params=pltpu.CompilerParams(vmem_limit_bytes=48 * 1024 * 1024),
    )(species, w, form_factor, g_vectors, pos, live)


def nonlocal_terms(proj_sums, occupied, strength):
    band_count = occupied.shape[0]
    atom_count = strength.shape[0]
    intersect = proj_sums[:, :band_count]
    weighted = intersect * occupied[None, :]
    energy_part = jnp.sum(strength.reshape(-1) * jnp.sum(weighted * intersect, axis=1))
    forces = []
    for axis_num in range(3):
        slope = proj_sums[:, (axis_num + 1) * band_count : (axis_num + 2) * band_count]
        per_row = jnp.sum(weighted * slope, axis=1).reshape(atom_count, PMAX)
        forces.append(-2.0 * jnp.sum(strength * per_row, axis=1))
    return (energy_part, jnp.stack(forces, axis=0))


def neb_project(
    force, here, prev_pos, next_pos, energy, prev_energy, next_energy, tangent_kind, is_climb
):
    to_next = next_pos - here
    from_prev = here - prev_pos
    rise_next = jnp.abs(next_energy - energy)
    rise_prev = jnp.abs(prev_energy - energy)
    larger = jnp.maximum(rise_next, rise_prev)
    smaller = jnp.minimum(rise_next, rise_prev)
    rising = next_energy > prev_energy
    weight_next = 1.0 + jnp.where(rising, larger, smaller)
    weight_prev = 1.0 + jnp.where(rising, smaller, larger)
    stiff_next = spring_constant * (1.0 + jax.nn.sigmoid(0.5 * (next_energy + energy)))
    stiff_prev = spring_constant * (1.0 + jax.nn.sigmoid(0.5 * (prev_energy + energy)))
    length_next = jnp.sqrt(jnp.sum(to_next * to_next, axis=(1, 2)) + 1.0)
    length_prev = jnp.sqrt(jnp.sum(from_prev * from_prev, axis=(1, 2)) + 1.0)
    upwind = weight_next[:, None, None] * to_next + weight_prev[:, None, None] * from_prev
    forward = to_next / length_next[:, None, None]
    backward = from_prev / length_prev[:, None, None]
    kind = tangent_kind[:, None, None]
    tangent = jnp.where(
        kind == 0,
        upwind,
        jnp.where(kind == 1, forward + backward, jnp.where(kind == 2, forward, backward)),
    )
    unit_tangent = tangent / jnp.sqrt(jnp.sum(tangent * tangent, axis=(1, 2)) + 1.0)[:, None, None]
    along = jnp.sum(force * unit_tangent, axis=(1, 2))[:, None, None]
    climbing = force - 2.0 * along * unit_tangent
    regular = (
        force
        - along * unit_tangent
        + (stiff_next * length_next - stiff_prev * length_prev)[:, None, None] * unit_tangent
    )
    return jnp.where(is_climb[:, None, None], climbing, regular)


def per_device(
    wave_coeffs,
    occupation,
    form_factor,
    g_vectors,
    species,
    proj_count,
    coupling,
    positions,
    energy_rest,
    force_rest,
    end_positions,
    end_energy,
    climb_index,
    tangent_kind,
):
    species_mask, strength = atom_tables(species, proj_count, coupling)
    occupied = occupation[0]
    local_atoms = ATOMS // lax.axis_size("ga")
    sums = projector_sums(
        wave_coeffs[0], form_factor, g_vectors, species, proj_count, positions[0]
    )
    proj_sums = lax.psum_scatter(sums, "ga", scatter_dimension=0, tiled=True)
    first_local = lax.axis_index("ga") * local_atoms
    strength_part = lax.dynamic_slice_in_dim(strength, first_local, local_atoms, 0)
    energy_part, force_part = nonlocal_terms(proj_sums, occupied, strength_part)
    force_full = lax.dynamic_update_slice_in_dim(
        jnp.zeros((3, ATOMS), jnp.float32), force_part, first_local, 1
    )
    force_nl, energy_nl = lax.psum((force_full, energy_part), ("band", "ga"))
    energy = energy_rest + energy_nl
    force = force_rest + force_nl[None, :, :]
    image_index = lax.axis_index("image")
    image_count = lax.axis_size("image")
    prev_pos, prev_energy = passed_along((positions, energy), "image", 1)
    next_pos, next_energy = passed_along((positions, energy), "image", -1)
    at_start = image_index == 0
    at_end = image_index == image_count - 1
    prev_pos = jnp.where(at_start, end_positions[:1], prev_pos)
    prev_energy = jnp.where(at_start, end_energy[:1], prev_energy)
    next_pos = jnp.where(at_end, end_positions[1:], next_pos)
    next_energy = jnp.where(at_end, end_energy[1:], next_energy)
    is_climb = climb_index == image_index
    neb_force = neb_project(
        force,
        positions,
        prev_pos,
        next_pos,
        energy,
        prev_energy,
        next_energy,
        tangent_kind,
        is_climb,
    )
    return (neb_force, energy)


def solution(mesh):
    in_specs = (
        P("image", "band", None, "ga"),
        P("image", "band"),
        P(None, None, "ga"),
        P(None, "ga"),
        P(),
        P(),
        P(),
        P("image", None, None),
        P("image"),
        P("image", None, None),
        P(),
        P(),
        P(),
        P("image"),
    )
    out_specs = (P("image", None, None), P("image"))
    return jax.shard_map(
        per_device, mesh=mesh, in_specs=in_specs, out_specs=out_specs, check_vma=False
    )
```
